256 devices in a mesh: parts: 4 (over y, x), dp: 64 (over z, core).
Axes of the slice: x: 2, y: 2, z: 32, core: 2. Of those that a mesh axis runs over, the one named last changes fastest.
The devices are a block of a 4x8x32 slice.
Arguments:
- activations: bfloat16 [65536, 14336], P(('parts', 'dp')), parts along dimension 0, may hold values from -6 to 6
- out_grads: bfloat16 [65536, 4096], P(('parts', 'dp')), parts along dimension 0, may hold values from -6 to 6
- lengths: int32 [256, 4], P(('parts', 'dp')), parts along dimension 0, may hold values from 1 to 128, 256 in all within a row
- proj_in: bfloat16 [14336, 64], replicated, may hold values from -0.046875 to 0.046875
- proj_out: bfloat16 [4096, 64], replicated, may hold values from -0.09375 to 0.09375
- queries: bfloat16 [8192, 4096], P(('parts', 'dp')), parts along dimension 0, may hold values from -0.01171875 to 0.01171875
Outputs:
- scores: bfloat16 [1024, 2048], P(('parts', 'dp')), parts along dimension 0
The draws below stay inside these ranges and needn't reach their ends.
There are 4 independent parts, one for each index of `parts`. The reference program is written for one: setup_inputs(seed, part) draws one part's arguments, and reference() takes and returns one part's arrays. A program takes and returns all parts, laid end to end along the dimension named above; an argument that names none is the same for every part. Nothing has to cross between parts.
Inputs may be any that keep to these rules, and one draw needn't show every extreme that they name: Each row of lengths sums to 256, and one entry of each row equals 128.
All inputs are finite; a program needn't handle non-finite values.
Results may differ from the reference program's by a relative error of at most 0.0065.
Values may be sent and summed in bfloat16 or wider, within the bound.
No kernel may reach another device: no remote copies, remote signals or barrier semaphores. Data moves between devices by JAX's collectives and lax.ppermute only.
A program may use at most 128 MiB of HBM per device.

```python
import math
import jax
import jax.numpy as jnp
import numpy as np

D = 4096
FF = 14336
RANK = 64
TOK_DEV = 256
EX_DEV = 4
TOKENS = 16384
N_TRAIN = 256
NQ = 2048
PARAMS = 4096
MOST = 128
N_DP = 64


def level_of(rng, dims, pieces, smallest, top_value):
    level = 1.0
    for dim, shards_of in pieces:
        heights = jax.random.uniform(jax.random.fold_in(jax.random.fold_in(rng, 6), dim), (shards_of,), jnp.float32, smallest / len(pieces), top_value / len(pieces))
        level = level * jnp.repeat(jnp.exp(heights), dims[dim] // shards_of).reshape((-1,) + (1,) * (len(dims) - 1 - dim))
    return level


def split_up(number_of, total, reach, lean):
    weights = [(1 << 20) // math.isqrt(standing ** lean) + 1 for standing in range(2, number_of + 1)]
    surplus, holding = total - reach - (number_of - 1), [1] * (number_of - 1)
    while surplus > 0:
        free = [i for i in range(number_of - 1) if holding[i] < reach]
        mass, remaining = sum([weights[i] for i in free]), surplus
        for i in free:
            more = min(reach - holding[i], max(1, remaining * weights[i] // mass), surplus)
            holding[i] = holding[i] + more
            surplus = surplus - more
    return np.array([reach] + holding)


def uneven(own_key, count, total, reach, lean):
    if count == 2:
        one = jax.random.randint(own_key, (), max(1, total - reach), min(reach, total - 1) + 1)
        return jnp.stack([one, total - one])
    sizes = jnp.asarray(split_up(count, total, reach, lean), jnp.int32)
    twos = (count - 1) // 2
    giver, sink = sizes[1:1 + 2 * twos:2], sizes[2:2 + 2 * twos:2]
    room = jnp.minimum(giver - 1, reach - sink)
    shifted = jax.random.randint(jax.random.fold_in(own_key, 1), (twos,), 0, 1 << 20) % (room + 1)
    sizes = sizes.at[1:1 + 2 * twos:2].set(giver - shifted).at[2:2 + 2 * twos:2].set(sink + shifted)
    return sizes[jax.random.permutation(jax.random.fold_in(own_key, 2), count)]


def scatter_about(own_key, extent, spread, reach, pieces=(), kind=jnp.bfloat16):
    entries = spread * jax.random.normal(own_key, extent, jnp.float32)
    if pieces:
        entries = entries * level_of(own_key, extent, pieces, -0.22, 0.18)
    return jnp.clip(entries, -reach, reach).astype(kind)


def setup_inputs(seed: int = 0, part: int = 0) -> dict:
    key_of = jax.random.split(jax.random.key(seed), 7)
    part_keys = jax.random.split(jax.random.fold_in(key_of[6], part), 7)
    activations = scatter_about(part_keys[0], (TOKENS, FF), 1.0, 6.0, ((0, 64),))
    out_grads = scatter_about(part_keys[1], (TOKENS, D), 1.0, 6.0, ((0, 64),))
    lengths = jax.vmap(lambda own: uneven(own, EX_DEV, TOK_DEV, MOST, 2))(jax.random.split(part_keys[2], N_DP)).reshape((N_DP, EX_DEV)).astype(jnp.int32)
    proj_in = scatter_about(key_of[3], (FF, RANK), FF ** -0.5, 0.046875)
    proj_out = scatter_about(key_of[4], (D, RANK), D ** -0.5, 0.09375)
    queries = scatter_about(part_keys[5], (NQ, PARAMS), (0.125 / RANK), 0.01171875, ((0, 64),))
    return dict(activations=activations, out_grads=out_grads, lengths=lengths, proj_in=proj_in, proj_out=proj_out, queries=queries)


def reference(activations, out_grads, lengths, proj_in, proj_out, queries):
    proj_acts = jnp.dot(activations, proj_in, preferred_element_type=jnp.float32).astype(jnp.bfloat16)
    proj_grads = jnp.dot(out_grads, proj_out, preferred_element_type=jnp.float32).astype(jnp.bfloat16)
    acts_wide = proj_acts.astype(jnp.float32)
    grads_wide = proj_grads.astype(jnp.float32)
    outer_terms = (grads_wide[:, :, None] * acts_wide[:, None, :]).reshape(TOKENS, RANK * RANK)
    tok_ends = jnp.cumsum(lengths.reshape(-1)).astype(jnp.int32)
    position = jnp.arange(TOKENS, dtype=jnp.int32)
    example_ids = jnp.searchsorted(tok_ends, position, side="right").astype(jnp.int32)
    example_grads = jax.ops.segment_sum(outer_terms, example_ids, num_segments=N_TRAIN).astype(jnp.bfloat16)
    return jnp.dot(example_grads, queries.T, preferred_element_type=jnp.float32).astype(jnp.bfloat16)
```

```python
import jax
import jax.numpy as jnp
from jax import lax
from jax.sharding import Mesh, PartitionSpec as P

DP = ("half", "side", "core")
HALF = "half"


def example_grads_of(activations, out_grads, lengths, proj_in, proj_out):
    tok_count = activations.shape[0]
    rank_size = proj_in.shape[1]
    proj_acts = jnp.dot(activations, proj_in, preferred_element_type=jnp.float32).astype(
        jnp.bfloat16
    )
    proj_grads = jnp.dot(out_grads, proj_out, preferred_element_type=jnp.float32).astype(
        jnp.bfloat16
    )
    counts = lengths[0]
    ex_count = counts.shape[0]
    tok_ends = jnp.sum(
        jnp.where(
            jnp.arange(ex_count)[:, None] >= jnp.arange(ex_count)[None, :], counts[None, :], 0
        ),
        axis=1,
    )
    tok_starts = tok_ends - counts
    position = jnp.arange(tok_count, dtype=jnp.int32)
    member = (
        (position[None, :] >= tok_starts[:, None]) & (position[None, :] < tok_ends[:, None])
    ).astype(jnp.bfloat16)
    masked_grads = member[:, :, None] * proj_grads[None, :, :]
    summed = jnp.einsum("eti,tj->eij", masked_grads, proj_acts, preferred_element_type=jnp.float32)
    return summed.reshape(ex_count, rank_size * rank_size).astype(jnp.bfloat16)


def local(activations, out_grads, lengths, proj_in, proj_out, queries):
    n_q = queries.shape[0]
    core = lax.axis_index("core")
    side = lax.axis_index("side")
    other = lax.ppermute(queries, "core", [(0, 1), (1, 0)])
    chip_q = jnp.concatenate(
        [jnp.where(core == 0, queries, other), jnp.where(core == 0, other, queries)], axis=0
    )
    beside = lax.ppermute(chip_q, "side", [(0, 1), (1, 0)])
    grads = example_grads_of(activations, out_grads, lengths, proj_in, proj_out)
    ex_count = grads.shape[0]
    gathered = lax.all_gather(grads, HALF, axis=0, tiled=True)
    contract = (((1,), (1,)), ((), ()))
    own = lax.dot_general(gathered, chip_q, contract, preferred_element_type=jnp.float32)
    far = lax.dot_general(gathered, beside, contract, preferred_element_type=jnp.float32)
    own, far = own.astype(jnp.bfloat16), far.astype(jnp.bfloat16)
    part = jnp.concatenate(
        [jnp.where(side == 0, own, far), jnp.where(side == 0, far, own)], axis=1
    )
    back = lax.all_to_all(
        part.reshape(-1, ex_count, 4 * n_q), HALF, split_axis=0, concat_axis=0, tiled=True
    )
    return back.transpose(1, 0, 2).reshape(ex_count, -1)


def solution(mesh):
    n_parts, n_dp = mesh.shape["parts"], mesh.shape["dp"]
    fine = Mesh(mesh.devices.reshape(n_parts, n_dp // 4, 2, 2), ("parts",) + DP)
    rows = P(("parts",) + DP, None)
    in_specs = (rows, rows, rows, P(), P(), rows)
    return jax.shard_map(local, mesh=fine, in_specs=in_specs, out_specs=rows, check_vma=False)
```

```python
import jax
import jax.numpy as jnp
from jax import lax
from jax.experimental import pallas as pl
from jax.experimental.pallas import tpu as pltpu
from jax.sharding import PartitionSpec as P


def example_grads_of(activations, out_grads, lengths, proj_in, proj_out):
    tok_count = activations.shape[0]
    rank_size = proj_in.shape[1]
    proj_acts = jnp.dot(activations, proj_in, preferred_element_type=jnp.float32).astype(
        jnp.bfloat16
    )
    proj_grads = jnp.dot(out_grads, proj_out, preferred_element_type=jnp.float32).astype(
        jnp.bfloat16
    )
    counts = lengths[0]
    ex_count = counts.shape[0]
    tok_ends = jnp.sum(
        jnp.where(
            jnp.arange(ex_count)[:, None] >= jnp.arange(ex_count)[None, :], counts[None, :], 0
        ),
        axis=1,
    )
    tok_starts = tok_ends - counts
    position = jnp.arange(tok_count, dtype=jnp.int32)
    member = (
        (position[None, :] >= tok_starts[:, None]) & (position[None, :] < tok_ends[:, None])
    ).astype(jnp.bfloat16)
    masked_grads = member[:, :, None] * proj_grads[None, :, :]
    summed = jnp.einsum("eti,tj->eij", masked_grads, proj_acts, preferred_element_type=jnp.float32)
    return summed.reshape(ex_count, rank_size * rank_size).astype(jnp.bfloat16)


def score_body(steps, place_ref, *refs):
    e_refs, w_refs, (mine_ref, theirs_ref) = refs[:4], refs[4 : 4 + 2 * steps], refs[4 + 2 * steps :]
    core = place_ref[1]
    ex = e_refs[0].shape[0]
    rows = jnp.concatenate([r[...] for r in e_refs], axis=0)
    contract = (((1,), (1,)), ((), ()))
    for s in range(steps):
        a = lax.dot_general(rows, w_refs[2 * s][...], contract, preferred_element_type=jnp.float32)
        b = lax.dot_general(
            rows, w_refs[2 * s + 1][...], contract, preferred_element_type=jnp.float32
        )
        first = jnp.where(core == 0, a, b)
        second = jnp.where(core == 0, b, a)
        both = jnp.concatenate([first, second], axis=1)
        slot = jnp.where(core == 0, steps - 1 - s, s)
        mine_ref[0, slot] = both[:ex]
        mine_ref[1, slot] = both[ex : 2 * ex]
        theirs_ref[0, slot] = both[2 * ex : 3 * ex]
        theirs_ref[1, slot] = both[3 * ex :]


def scores_of(place, e_blocks, w_blocks):
    steps = len(w_blocks) // 2
    ex, nq = e_blocks[0].shape[0], w_blocks[0].shape[0]
    shape = jax.ShapeDtypeStruct((2, steps, ex, 2 * nq), jnp.float32)
    vmem = pl.BlockSpec(memory_space=pltpu.VMEM)
    return pl.pallas_call(
        lambda *refs: score_body(steps, *refs),
        out_shape=(shape, shape),
        in_specs=[pl.BlockSpec(memory_space=pltpu.SMEM)] + [vmem] * (4 + 2 * steps),
        out_specs=(vmem, vmem),
        name="window_scores",
    )(place, *e_blocks, *w_blocks)


def place_body(n_chip, steps, place_ref, kf_ref, kn_ref, gf_ref, gn_ref, out_ref, hold_ref):
    chip, core = place_ref[0], place_ref[1]
    half = kf_ref.shape[2] // 2
    for n, (ref, rows, ahead, order) in enumerate(
        (
            (kn_ref, 0, core == 0, core),
            (kf_ref, 0, core == 0, core),
            (gn_ref, half, core == 1, 1 - core),
            (gf_ref, half, core == 1, 1 - core),
        )
    ):
        far = n % 2
        where = jnp.where(ahead, far, 3 - far)
        for h in range(2):
            for t in range(steps):
                at = where * (2 * steps) + jnp.where(order == 0, h, 1 - h) * steps + t
                hold_ref[at] = ref[h, t, rows : rows + half]
    for j in range(0, n_chip, 2):
        pair = [hold_ref[lax.rem(j + k - chip + n_chip, n_chip)] for k in range(2)]
        wide = pair[0].shape[1]
        out_ref[:, j * wide : (j + 2) * wide] = jnp.concatenate(pair, axis=1).astype(out_ref.dtype)


def placed(place, n_chip, steps, kept_far, kept_near, got_far, got_near):
    half, wide = kept_far.shape[2] // 2, kept_far.shape[3]
    vmem = pl.BlockSpec(memory_space=pltpu.VMEM)
    return pl.pallas_call(
        lambda *refs: place_body(n_chip, steps, *refs),
        out_shape=jax.ShapeDtypeStruct((half, n_chip * wide), jnp.bfloat16),
        in_specs=[pl.BlockSpec(memory_space=pltpu.SMEM)] + [vmem] * 4,
        out_specs=vmem,
        scratch_shapes=[pltpu.VMEM((n_chip, half, wide), jnp.float32)],
        name="place_scores",
    )(place, kept_far, kept_near, got_far, got_near)


def solution(mesh):
    n_dp = mesh.shape["dp"]
    n_chip = n_dp // 2
    quarter = n_chip // 4
    steps = near = quarter // 2
    far = quarter + near
    sibling = [(p, p ^ 1) for p in range(n_dp)]

    def shifted(d0, d1):
        pairs = []
        for z in range(n_chip):
            pairs.append((2 * z, 2 * ((z + d0) % n_chip)))
            pairs.append((2 * z + 1, 2 * ((z + d1) % n_chip) + 1))
        return pairs

    def send(x, d0, d1):
        return lax.ppermute(x, "dp", shifted(d0, d1))

    def swap(x):
        return lax.ppermute(x, "dp", sibling)

    def local(activations, out_grads, lengths, proj_in, proj_out, queries):
        where = lax.axis_index("dp").astype(jnp.int32)
        place = jnp.stack([where >> 1, where & 1])
        a, b = queries, swap(queries)
        windows = []
        for s in range(steps):
            a = send(a, 1, -1 if s else 0)
            b = send(b, 1, -1 if s else 0)
            windows += [a, b]
        grads = example_grads_of(activations, out_grads, lengths, proj_in, proj_out)
        chip_grads = jnp.concatenate([grads, swap(grads)], axis=0)
        e_far = send(chip_grads, far, -far)
        e_near = send(chip_grads, near, -near)
        mine, theirs = scores_of(place, [e_far, e_near, swap(e_far), swap(e_near)], windows)
        full = jnp.concatenate([mine, swap(theirs)], axis=1)
        full = full.reshape((2, 2) + mine.shape[1:])
        kept_far = send(full[0], -far, far)
        kept_near = send(full[1], -near, near)
        return placed(place, n_chip, steps, kept_far, kept_near, swap(kept_far), swap(kept_near))

    rows = P(("parts", "dp"), None)
    in_specs = (rows, rows, rows, P(), P(), rows)
    return jax.shard_map(local, mesh=mesh, in_specs=in_specs, out_specs=rows, check_vma=False)
```
